32 devices in a mesh: gx: 4 (over z), gy: 4 (over y, x), gz: 2 (over core).
Axes of the slice: x: 2, y: 2, z: 4, core: 2. Of those that a mesh axis runs over, the one named last changes fastest.
Arguments:
- forces: float32 [3, 64, 64, 256], P(None, 'gx', 'gy', 'gz'), may hold values from -8 to 8
- mass_shift: float32 [64, 64, 256], P('gx', 'gy', 'gz'), may hold values from 0.5 to 2
- deflation: float32 [16, 3, 64, 64, 256], P(None, None, 'gx', 'gy', 'gz'), may hold values from -0.01953125 to 0.01953125
- coarse_factor: float32 [512, 512], P('gz'), may hold values from -0.041033009 to 0.6, as said below
- coarse_slot: int32 [32], replicated, may hold values from 0 to 31, each once
Outputs:
- solution: float32 [3, 64, 64, 256], P(None, 'gx', 'gy', 'gz')
- residual: float32 [3, 64, 64, 256], P(None, 'gx', 'gy', 'gz')
- direction: float32 [3, 64, 64, 256], P(None, 'gx', 'gy', 'gz')
The draws below stay inside these ranges and needn't reach their ends.
Inputs may be any that keep to these rules, and one draw needn't show every extreme that they name: `coarse_factor`: lower triangular: zero above the diagonal; diagonal entries between 0.3 and 0.6. `coarse_slot`: each subdomain has its own coarse position.
All inputs are finite; a program needn't handle non-finite values.
Results may differ from the reference program's by a relative error of at most 0.0003.
Values sent between devices are 32-bit elements; how exact they have to be, the bound alone decides.
A program may use at most 192 MiB of HBM per device.

```python
import math
import jax
import jax.numpy as jnp
from jax import lax

CX = 16
CY = 16
CZ = 128
K = 16
SWEEPS = 3
ITERS = 4
NX = 64
NY = 64
NZ = 256
SUBS = 32
NC = 512
N_GX = 4
N_GY = 4
N_GZ = 2


lower_offset = 0.012


def draw_forces(key, part):
    key_field = jax.random.fold_in(key, 3)
    along_x = (jnp.arange(NX, dtype=jnp.float32) + 0.5) / NX
    along_y = (jnp.arange(NY, dtype=jnp.float32) + 0.5) / NY
    along_z = (jnp.arange(NZ, dtype=jnp.float32) + 0.5) / NZ
    ramp_sum = along_x[:, None, None] + along_y[None, :, None] + along_z[None, None, :]
    rough_part = jax.random.truncated_normal(key_field, -4.0, 4.0, (3, NX, NY, NZ), jnp.float32)
    return rough_part * 3.0 ** (ramp_sum / 6.0)


def draw_coarse_factor(key, part):
    key_lower, key_diag = jax.random.split(jax.random.fold_in(key, 5))
    spread = 0.3 / math.sqrt(NC)
    lower_part = jax.random.truncated_normal(key_lower, -4.0, 4.0, (NC, NC), jnp.float32) * spread
    lower_part = lower_part + lower_offset
    diagonal = jax.random.uniform(key_diag, (NC,), jnp.float32, 0.3, 0.6)
    return jnp.tril(lower_part, -1) + jnp.diag(diagonal)


def level_of(key, extent, pieces, least, high):
    factor_of = 1.0
    for dim, blocks in pieces:
        steps = jax.random.uniform(jax.random.fold_in(jax.random.fold_in(key, 6), dim), (blocks,), jnp.float32, least / len(pieces), high / len(pieces))
        factor_of = factor_of * jnp.repeat(jnp.exp(steps), extent[dim] // blocks).reshape((-1,) + (1,) * (len(extent) - 1 - dim))
    return factor_of


def scatter_about(stream_key, dims, deviation, bound, cuts=(), kind=jnp.bfloat16):
    entries = deviation * jax.random.normal(stream_key, dims, jnp.float32)
    if cuts:
        entries = entries * level_of(stream_key, dims, cuts, -0.22, 0.18)
    return jnp.clip(entries, -bound, bound).astype(kind)


def setup_inputs(seed: int = 0) -> dict:
    keys = jax.random.split(jax.random.key(seed), 6)
    return {
        "forces": draw_forces(jax.random.fold_in(keys[5], 71), 0),
        "mass_shift": jnp.clip(jnp.exp(math.log(2.0) - 1.3862944 * jax.random.uniform(keys[1], (NX, NY, NZ), jnp.float32) ** level_of(keys[1], (NX, NY, NZ), ((0, 4), (1, 4), (2, 2)), -0.2, 0.2)), 0.5, 2.0),
        "deflation": scatter_about(keys[2], (K, 3, NX, NY, NZ), ((3 * CX * CY * CZ) ** -0.5), 0.01953125, ((2, 4), (3, 4), (4, 2)), jnp.float32),
        "coarse_factor": draw_coarse_factor(jax.random.fold_in(keys[5], 71), 0),
        "coarse_slot": jax.random.permutation(keys[4], SUBS).astype(jnp.int32),
    }


shear_modulus = 0.25
lame_first = 0.375
relaxation = 0.6
offsets_unit = ((1, 0, 0), (0, 1, 0), (0, 0, 1))

def stencil(padded, mass_shift):
    size_x = padded.shape[1] - 2
    size_y = padded.shape[2] - 2
    size_z = padded.shape[3] - 2
    stiffer = lame_first + shear_modulus

    def neighbor(component, shift_x, shift_y, shift_z):
        return padded[component, 1 + shift_x:1 + shift_x + size_x, 1 + shift_y:1 + shift_y + size_y, 1 + shift_z:1 + shift_z + size_z]

    def moved(component, first_unit, second_unit, sign_first, sign_second):
        return neighbor(component, sign_first * first_unit[0] + sign_second * second_unit[0], sign_first * first_unit[1] + sign_second * second_unit[1], sign_first * first_unit[2] + sign_second * second_unit[2])
    outputs = []
    for component in range(3):
        middle = neighbor(component, 0, 0, 0)
        summed = mass_shift * middle
        for axis_number in range(3):
            unit_step = offsets_unit[axis_number]
            second_diff = moved(component, unit_step, unit_step, 1, 0) + moved(component, unit_step, unit_step, -1, 0) - 2.0 * middle
            weight = shear_modulus + stiffer if axis_number == component else shear_modulus
            summed = summed - weight * second_diff
        own_unit = offsets_unit[component]
        for partner in range(3):
            if partner != component:
                partner_unit = offsets_unit[partner]
                mixed_term = moved(partner, own_unit, partner_unit, 1, 1) - moved(partner, own_unit, partner_unit, 1, -1) - moved(partner, own_unit, partner_unit, -1, 1) + moved(partner, own_unit, partner_unit, -1, -1)
                summed = summed - 0.25 * stiffer * mixed_term
        outputs.append(summed)
    return jnp.stack(outputs)

def reference(forces, mass_shift, deflation, coarse_factor, coarse_slot):
    diagonal = mass_shift + (6.0 * shear_modulus + 2.0 * (lame_first + shear_modulus))
    blocked_shape = (3, N_GX, CX, N_GY, CY, N_GZ, CZ)

    def operate(field):
        return stencil(jnp.pad(field, ((0, 0), (1, 1), (1, 1), (1, 1))), mass_shift)

    def restrict(field):
        blocked = field.reshape(blocked_shape)

        def one_vector(vector):
            return jnp.sum(vector.reshape(blocked_shape) * blocked, axis=(0, 2, 4, 6))
        sums = lax.map(one_vector, deflation)
        return jnp.transpose(sums, (1, 2, 3, 0)).reshape(N_GX * N_GY * N_GZ, K)

    def prolong(weights):
        grid = jnp.transpose(weights.reshape(N_GX, N_GY, N_GZ, K), (3, 0, 1, 2))

        def add_vector(summed, pair):
            vector, scales = pair
            return (summed + vector.reshape(blocked_shape) * scales[None, :, None, :, None, :, None], None)
        start = jnp.zeros(blocked_shape, jnp.float32)
        summed, ignored = lax.scan(add_vector, start, (deflation, grid))
        return summed.reshape(3, NX, NY, NZ)

    def precondition(field):
        restricted = restrict(field)
        ordered = jnp.zeros_like(restricted).at[coarse_slot].set(restricted).reshape(-1)
        forward = jax.scipy.linalg.solve_triangular(coarse_factor, ordered, lower=True)
        coarse = jax.scipy.linalg.solve_triangular(coarse_factor, forward, lower=True, trans=1)
        correction = prolong(coarse.reshape(-1, K)[coarse_slot])
        smooth = jnp.zeros_like(field)
        for sweep_index in range(SWEEPS):
            smooth = smooth + relaxation * (field - operate(smooth)) / diagonal
        return correction + smooth
    solution = jnp.zeros_like(forces)
    residual = forces
    direction = forces
    precond_prior = jnp.float32(1.0)
    for iteration in range(ITERS):
        preconditioned = precondition(residual)
        precond_norm = jnp.sum(residual * preconditioned)
        if iteration == 0:
            direction = preconditioned
        else:
            direction = preconditioned + precond_norm / precond_prior * direction
        image_field = operate(direction)
        step_size = precond_norm / jnp.sum(direction * image_field)
        solution = solution + step_size * direction
        residual = residual - step_size * image_field
        precond_prior = precond_norm
    return (solution, residual, direction)
```

```python
import functools

import jax
import jax.numpy as jnp
from jax import lax
from jax.experimental import pallas as pl
from jax.experimental.pallas import tpu as pltpu
from jax.sharding import PartitionSpec as P

SWEEPS = 3
ITERS = 4
MESH = pl.DeviceIdType.MESH
HIGHEST = lax.Precision.HIGHEST
W = 3
LEAD = 4
DIRS = tuple((dx, dy) for dx in (-1, 0, 1) for dy in (-1, 0, 1) if (dx, dy) != (0, 0))
BLOCK = 128


def dot(a, b):
    return jnp.dot(a, b, precision=HIGHEST, preferred_element_type=jnp.float32)


def kernel(
    sizes,
    forces, mass, defl, factor, slot_column,
    sol, res, direc,
    zext, rext, idir, cext, mext, cor, ua, ub, uz, vx,
    low, high, got_low, got_high,
    low_c, high_c, got_low_c, got_high_c,
    low_m, high_m, got_low_m, got_high_m,
    zsend, zgot, vzb,
    full, inv, sol_mat, gsend, gat, gres, gdir,
    zx_send, zx_recv, c_send, c_recv, m_send, m_recv,
    zc_send, zc_recv, g_send, g_recv, f_send, f_recv, f_local,
):
    nx, ny, nz, cx, cy, vectors, order = sizes
    n = nx * ny * nz
    ex = cx + 2 * LEAD
    ey = cy + 8
    gx, gy, gz = lax.axis_index("gx"), lax.axis_index("gy"), lax.axis_index("gz")
    me = (gx * ny + gy) * nz + gz
    f32 = jnp.float32

    def coords(t):
        return {"gx": t // (ny * nz), "gy": (t // nz) % ny, "gz": t % nz}

    lane = lax.broadcasted_iota(jnp.int32, (ey, 128), 1)
    row8 = lax.broadcasted_iota(jnp.int32, (8, 128), 0)
    rows = lax.broadcasted_iota(jnp.int32, (ey, 128), 0)
    lane1 = lax.broadcasted_iota(jnp.int32, (1, 128), 1)

    for ref in (zext, cor, mext, got_low, got_high, got_low_c, got_high_c, got_low_m, got_high_m):
        lead = ref.shape[0]
        for c in range(lead):
            def clear(i, _, ref=ref, c=c):
                ref[c, i] = jnp.zeros(ref.shape[2:], f32)
                return 0
            lax.fori_loop(0, ref.shape[1], clear, 0)
    zgot[...] = jnp.zeros(zgot.shape, f32)

    barrier = pltpu.get_barrier_semaphore()

    def greet(j, _):
        t = lax.rem(me + j, n)
        pl.semaphore_signal(barrier, inc=1, device_id=coords(t), device_id_type=MESH)
        return 0

    lax.fori_loop(1, n, greet, 0)
    pl.semaphore_wait(barrier, n - 1)

    slab = order // nz

    def slab_copy(j):
        t = lax.rem(gz + j, nz)
        return pltpu.make_async_remote_copy(
            src_ref=factor,
            dst_ref=full.at[gz],
            send_sem=f_send.at[j - 1],
            recv_sem=f_recv.at[j - 1],
            device_id={"gx": gx, "gy": gy, "gz": t},
            device_id_type=MESH,
        )

    for j in range(1, nz):
        slab_copy(j).start()
    own_slab = pltpu.make_async_copy(factor, full.at[gz], f_local)
    own_slab.start()

    def exists(dx, dy):
        ok = jnp.bool_(True)
        if dx < 0:
            ok = jnp.logical_and(ok, gx > 0)
        if dx > 0:
            ok = jnp.logical_and(ok, gx < nx - 1)
        if dy < 0:
            ok = jnp.logical_and(ok, gy > 0)
        if dy > 0:
            ok = jnp.logical_and(ok, gy < ny - 1)
        return ok

    def pieces(ext, lo, hi, glo, ghi, send, recv):
        half = cx // 2
        out = []
        for d, (dx, dy) in enumerate(DIRS):
            if dy == 0:
                src = ext.at[:, pl.ds(LEAD if dx < 0 else LEAD + cx - W, W), pl.ds(0, cy)]
                dst = ext.at[:, pl.ds(LEAD + cx if dx < 0 else LEAD - W, W), pl.ds(0, cy)]
            else:
                start, count = {0: (0, half), -1: (0, 2), 1: (half - 2, 2)}[dx]
                to = {0: 2, -1: 2 + half, 1: 0}[dx]
                src = (lo if dy < 0 else hi).at[:, pl.ds(start, count)]
                dst = (glo if dy < 0 else ghi).at[:, pl.ds(to, count)]
            copy = pltpu.make_async_remote_copy(
                src_ref=src,
                dst_ref=dst,
                send_sem=send.at[d],
                recv_sem=recv.at[d],
                device_id={"gx": gx + dx, "gy": gy + dy, "gz": gz},
                device_id_type=MESH,
            )
            out.append((dx, dy, copy))
        return out

    def send_halo(ext, lo, hi, glo, ghi, send, recv):
        def pack(i, _):
            for c in range(ext.shape[0]):
                even, odd = LEAD + 2 * i, LEAD + 2 * i + 1
                lo[c, i] = jnp.where(row8 < 4, ext[c, even, 0:8], pltpu.roll(ext[c, odd, 0:8], 4, 0))
                hi[c, i] = jnp.where(
                    row8 >= 4, ext[c, even, cy - 8 : cy], pltpu.roll(ext[c, odd, cy - 8 : cy], 4, 0)
                )
            return 0

        lax.fori_loop(0, cx // 2, pack, 0)
        for dx, dy, copy in pieces(ext, lo, hi, glo, ghi, send, recv):
            pl.when(exists(dx, dy))(copy.start)

    def take_halo(ext, lo, hi, glo, ghi, send, recv):
        for dx, dy, copy in pieces(ext, lo, hi, glo, ghi, send, recv):
            pl.when(exists(-dx, -dy))(copy.wait_recv)
            pl.when(exists(dx, dy))(copy.wait_send)

        def unpack(i, _):
            for c in range(ext.shape[0]):
                a, b = glo[c, i], ghi[c, i]
                ext[c, 2 * i, cy : cy + 8] = jnp.where(row8 < 4, a, b)
                ext[c, 2 * i + 1, cy : cy + 8] = jnp.where(
                    row8 < 4, pltpu.roll(a, 4, 0), pltpu.roll(b, 4, 0)
                )
            return 0

        lax.fori_loop(0, ex // 2, unpack, 0)

    halo_z = (zext, low, high, got_low, got_high, zx_send, zx_recv)
    halo_c = (cor, low_c, high_c, got_low_c, got_high_c, c_send, c_recv)
    halo_m = (mext, low_m, high_m, got_low_m, got_high_m, m_send, m_recv)

    def columns(stage, side):
        return pltpu.make_async_remote_copy(
            src_ref=zsend.at[stage, side],
            dst_ref=zgot.at[stage, 1 - side],
            send_sem=zc_send.at[stage, side],
            recv_sem=zc_recv.at[stage, side],
            device_id={"gx": gx, "gy": gy, "gz": gz + (2 * side - 1)},
            device_id_type=MESH,
        )

    has = (gz > 0, gz < nz - 1)

    def exchange_columns(u, stage, first, last):
        for side in (0, 1):
            @pl.when(has[side])
            def _(side=side):
                def gather(x, acc):
                    shift = x if side == 0 else x + 1
                    return tuple(
                        jnp.where(lane == x, pltpu.roll(u[c, x], shift, 1), acc[c]) for c in range(3)
                    )

                acc = lax.fori_loop(first, last, gather, (jnp.zeros((ey, 128), f32),) * 3, unroll=2)
                for c in range(3):
                    zsend[stage, side, c] = acc[c]
                columns(stage, side).start()
        for side in (0, 1):
            pl.when(has[1 - side])(columns(stage, side).wait_recv)
            pl.when(has[side])(columns(stage, side).wait_send)
        for side in (0, 1):
            bx, by = zgot[stage, side, 0], zgot[stage, side, 1]
            vzb[side] = (
                pltpu.roll(bx, 127, 1) - pltpu.roll(bx, 1, 1)
                + pltpu.roll(by, ey - 1, 0) - pltpu.roll(by, 1, 0)
            )

    def y_pair(v):
        return pltpu.roll(v, ey - 1, 0), pltpu.roll(v, 1, 0)

    def z_pair(v, upper, lower, x):
        up = jnp.where(lane == 127, pltpu.roll(upper, 127 - x, 1), pltpu.roll(v, 127, 1))
        down = jnp.where(lane == 0, pltpu.roll(lower, 128 - x, 1), pltpu.roll(v, 1, 1))
        return up, down

    def off_diagonal(u, stage, first, last, use, carry):
        def before(x, _):
            p, m = y_pair(u[1, x])
            q, r = z_pair(u[2, x], zgot[stage, 1, 2], zgot[stage, 0, 2], x)
            vx[x] = (p - m) + (q - r)
            return 0

        lax.fori_loop(first - 1, last + 1, before, 0, unroll=2)

        def at(x, carry):
            pair, diff = [], []
            for c in range(3):
                v = u[c, x]
                xp, xm = u[c, x + 1], u[c, x - 1]
                yp, ym = y_pair(v)
                zp, zm = z_pair(v, zgot[stage, 1, c], zgot[stage, 0, c], x)
                pair.append((xp + xm, yp + ym, zp + zm))
                diff.append(((xp - xm), (yp - ym), (zp - zm))[c])
            px, py, pz = diff
            dx = vx[x + 1] - vx[x - 1]
            yp, ym = y_pair(px + pz)
            zp, zm = z_pair(px + py, vzb[1], vzb[0], x)
            mixed = (dx, yp - ym, zp - zm)
            off = tuple(
                0.25 * (pair[c][0] + pair[c][1] + pair[c][2]) + 0.625 * pair[c][c] + 0.15625 * mixed[c]
                for c in range(3)
            )
            return use(x, off, carry)

        return lax.fori_loop(first, last, at, carry)

    base = lax.rem(me, 8) * vectors if vectors * 8 == 128 else 0

    def share(slot, gamma, energy):
        def part(x, acc):
            acc = list(acc)
            for c in range(3):
                v = zext[c, LEAD + x, 0:cy]
                for k in range(vectors):
                    prod = defl[k, c, x] * v
                    for t in range(0, cy, 8):
                        acc[k] = acc[k] + prod[t : t + 8]
            return tuple(acc)

        acc = lax.fori_loop(0, cx, part, (jnp.zeros((8, 128), f32),) * vectors)
        line = jnp.zeros((1, 128), f32)
        for k in range(vectors):
            total = jnp.sum(jnp.sum(acc[k], axis=0, keepdims=True), axis=1, keepdims=True)
            line = jnp.where(lane1 == base + k, total, line)
        gsend[slot, 0:1] = line
        gsend[slot, 1:2] = jnp.where(lane1 == 0, gamma, jnp.where(lane1 == 1, energy, 0.0))
        gat[slot, me] = gsend[slot]

        def push(j, _):
            t = lax.rem(me + j, n)
            pltpu.make_async_remote_copy(
                src_ref=gsend.at[slot],
                dst_ref=gat.at[slot, me],
                send_sem=g_send.at[slot],
                recv_sem=g_recv.at[slot, me],
                device_id=coords(t),
                device_id_type=MESH,
            ).start()
            return 0

        lax.fori_loop(1, n, push, 0)

    def collect(slot):
        def await_one(j, _):
            t = lax.rem(me + j, n)
            pltpu.make_async_copy(gsend.at[slot], gat.at[slot, t], g_recv.at[slot, t]).wait()
            return 0

        lax.fori_loop(1, n, await_one, 0)
        pltpu.make_async_copy(
            gat.at[slot, pl.ds(0, n - 1)], gat.at[slot, pl.ds(0, n - 1)], g_send.at[slot]
        ).wait()
        lines, scal = [], jnp.zeros((1, 128), f32)
        for t in range(n // 8):
            both = jnp.zeros((2, 128), f32)
            for s in range(8):
                both = both + gat[slot, 8 * t + s]
            lines.append(both[0:1])
            scal = scal + both[1:2]
        gamma = jnp.sum(jnp.where(lane1 == 0, scal, 0.0), axis=1, keepdims=True)
        energy = jnp.sum(jnp.where(lane1 == 1, scal, 0.0), axis=1, keepdims=True)
        return lines, gamma, energy

    def fill(x, _):
        for c in range(3):
            zext[c, LEAD + x, 0:cy] = forces[c, x]
            sol[c, x] = jnp.zeros((cy, 128), f32)
            direc[c, x] = jnp.zeros((cy, 128), f32)
        mext[0, LEAD + x, 0:cy] = mass[x]
        return 0

    lax.fori_loop(0, cx, fill, 0)
    send_halo(*halo_z)
    send_halo(*halo_m)
    zero = jnp.zeros((1, 1), f32)
    share(0, zero, zero)

    for j in range(1, nz):
        copy = slab_copy(j)
        copy.wait_recv()
        copy.wait_send()
    own_slab.wait()
    per_slab = slab // BLOCK
    blocks = order // BLOCK
    group = min(4, blocks)
    r_i = lax.broadcasted_iota(jnp.int32, (BLOCK, BLOCK), 0)
    c_i = lax.broadcasted_iota(jnp.int32, (BLOCK, BLOCK), 1)

    def invert(g, _):
        lows, xs = [], []
        for q in range(group):
            i = g * group + q
            at = pl.ds(pl.multiple_of((i % per_slab) * BLOCK, BLOCK), BLOCK)
            col = pl.ds(pl.multiple_of(i * BLOCK, BLOCK), BLOCK)
            block = full[i // per_slab, at, col]
            lows.append(block)
            xs.append(jnp.where(r_i == c_i, 1.0 / jnp.where(r_i == c_i, block, 1.0), 0.0))
        s = 1
        while s < BLOCK:
            pick = (r_i // (2 * s) == c_i // (2 * s)) & ((r_i // s) % 2 == 1) & ((c_i // s) % 2 == 0)
            mids = [dot(jnp.where(pick, lows[q], 0.0), xs[q]) for q in range(group)]
            xs = [xs[q] - dot(xs[q], mids[q]) for q in range(group)]
            s *= 2
        for q in range(group):
            inv[g * group + q] = xs[q]
        return 0

    lax.fori_loop(0, blocks // group, invert, 0)

    width = min(512, order)

    def wipe(i, _):
        sol_mat[pl.ds(pl.multiple_of(i * 8, 8), 8), :] = jnp.zeros((8, order), f32)
        return 0

    lax.fori_loop(0, order // 8, wipe, 0)
    w_rows = lax.broadcasted_iota(jnp.int32, (BLOCK, width), 0)

    def substitute(i, _):
        at = pl.ds(pl.multiple_of((i % per_slab) * BLOCK, BLOCK), BLOCK)

        def over(j, _):
            col = pl.ds(pl.multiple_of(j * width, width), width)
            right = jnp.where(w_rows + i * BLOCK == slot_column[:, col], 1.0, 0.0)
            right = right - dot(full[i // per_slab, at, :], sol_mat[:, col])
            sol_mat[pl.ds(pl.multiple_of(i * BLOCK, BLOCK), BLOCK), col] = dot(inv[i], right)
            return 0

        lax.fori_loop(0, order // width, over, 0)
        return 0

    lax.fori_loop(0, blocks, substitute, 0)

    take_halo(*halo_z)
    take_halo(*halo_m)
    y_ok = (rows < cy) | ((rows < cy + 4) & (gy < ny - 1)) | ((rows >= cy + 4) & (gy > 0))

    def settle(x, _):
        x_ok = ((x >= LEAD) | (gx > 0)) & ((x < LEAD + cx) | (gx < nx - 1))
        keep = jnp.where(x_ok, 1.0, 0.0)
        cext[x] = jnp.where(y_ok, 0.6 / (mext[0, x] + 2.75), 0.0) * keep
        for c in range(3):
            rext[c, x] = zext[c, x]
            idir[c, x] = jnp.zeros((ey, 128), f32)
        return 0

    lax.fori_loop(0, ex, settle, 0)
    lines, _, _ = collect(0)
    for t in range(n // 8):
        gres[t] = lines[t]
        gdir[t] = jnp.zeros((1, 128), f32)

    strip = 64

    def coarse():
        own = pl.ds(pl.multiple_of((me // 8) * 128, 128), 128)

        def some(i, acc):
            at = pl.ds(pl.multiple_of(i * strip, strip), strip)
            y = jnp.zeros((strip, 128), f32)
            for t in range(order // 128):
                y = y + sol_mat[at, t * 128 : (t + 1) * 128] * gres[t]
            y = jnp.sum(y, axis=1, keepdims=True)
            return acc + jnp.sum(y * sol_mat[at, own], axis=0, keepdims=True)

        line = lax.fori_loop(0, order // strip, some, jnp.zeros((1, 128), f32), unroll=2)
        weights = [
            jnp.sum(jnp.where(lane1 == base + k, line, 0.0), axis=1, keepdims=True)
            for k in range(vectors)
        ]
        spread = [jnp.broadcast_to(w, (8, 128)) for w in weights]

        def correct(x, _):
            for c in range(3):
                for t in range(0, cy, 8):
                    acc = spread[0] * defl[0, c, x, t : t + 8]
                    for k in range(1, vectors):
                        acc = acc + spread[k] * defl[k, c, x, t : t + 8]
                    cor[c, LEAD + x, t : t + 8] = acc
            return 0

        lax.fori_loop(0, cx, correct, 0)

    def iterate(it, carry):
        gamma_prior, step_prior = carry
        slot = lax.rem(it + 1, 2)
        coarse()
        send_halo(*halo_c)

        def start(x, _):
            for c in range(3):
                ua[c, x] = cext[x] * rext[c, x]
            return 0

        lax.fori_loop(LEAD - 3, LEAD + cx + 3, start, 0)

        def sweep(src, dst):
            def use(x, off, carry):
                for c in range(3):
                    dst[c, x] = 0.4 * src[c, x] + cext[x] * (rext[c, x] + off[c])
                return carry
            return use

        exchange_columns(ua, 0, LEAD - 3, LEAD + cx + 3)
        off_diagonal(ua, 0, LEAD - 2, LEAD + cx + 2, sweep(ua, ub), 0)
        exchange_columns(ub, 1, LEAD - 2, LEAD + cx + 2)
        off_diagonal(ub, 1, LEAD - 1, LEAD + cx + 1, sweep(ub, uz), 0)
        take_halo(*halo_c)

        def join(x, _):
            for c in range(3):
                uz[c, x] = uz[c, x] + cor[c, x]
            return 0

        lax.fori_loop(LEAD - 1, LEAD + cx + 1, join, 0)
        exchange_columns(uz, 2, LEAD - 1, LEAD + cx + 1)

        def image(x, off, carry):
            gam, ene = carry
            diag = mext[0, x, 0:cy] + 2.75
            for c in range(3):
                z = uz[c, x, 0:cy]
                a = diag * z - off[c][0:cy]
                zext[c, x, 0:cy] = a
                gam = gam + rext[c, x, 0:cy] * z
                ene = ene + z * a
            return gam, ene

        nothing = jnp.zeros((cy, 128), f32)
        gam, ene = off_diagonal(uz, 2, LEAD, LEAD + cx, image, (nothing, nothing))
        gam = jnp.sum(jnp.sum(gam, axis=0, keepdims=True), axis=1, keepdims=True)
        ene = jnp.sum(jnp.sum(ene, axis=0, keepdims=True), axis=1, keepdims=True)

        @pl.when(it < ITERS - 1)
        def _():
            send_halo(*halo_z)

        share(slot, gam, ene)
        lines, gamma, energy = collect(slot)
        momentum = jnp.where(it == 0, 0.0, gamma / gamma_prior)
        step = gamma / (energy - momentum * gamma / step_prior)

        @pl.when(it < ITERS - 1)
        def _():
            take_halo(*halo_z)

        def update(x, _):
            for c in range(3):
                image_dir = zext[c, x] + momentum * idir[c, x]
                idir[c, x] = image_dir
                rext[c, x] = rext[c, x] - step * image_dir
            return 0

        lax.fori_loop(LEAD - 3, LEAD + cx + 3, update, 0)

        def advance(x, _):
            for c in range(3):
                d = uz[c, LEAD + x, 0:cy] + momentum * direc[c, x]
                direc[c, x] = d
                sol[c, x] = sol[c, x] + step * d
            return 0

        lax.fori_loop(0, cx, advance, 0)
        for t in range(n // 8):
            image_line = lines[t] + momentum * gdir[t]
            gdir[t] = image_line
            gres[t] = gres[t] - step * image_line
        return gamma, step

    one = jnp.ones((1, 1), f32)
    lax.fori_loop(0, ITERS, iterate, (one, one))

    def give(x, _):
        for c in range(3):
            res[c, x] = rext[c, LEAD + x, 0:cy]
        return 0

    lax.fori_loop(0, cx, give, 0)


def solution(mesh):
    nx, ny, nz = mesh.shape["gx"], mesh.shape["gy"], mesh.shape["gz"]

    def body(forces, mass_shift, deflation, coarse_factor, coarse_slot):
        vectors = deflation.shape[0]
        cx, cy = forces.shape[1], forces.shape[2]
        order = coarse_factor.shape[1]
        slab = coarse_factor.shape[0]
        n = nx * ny * nz
        slot_column = (
            coarse_slot[:, None] * vectors + jnp.arange(vectors, dtype=jnp.int32)[None, :]
        ).reshape(1, -1)
        ex, ey = cx + 2 * LEAD, cy + 8
        f32 = jnp.float32
        vm = lambda *shape: pltpu.VMEM(shape, f32)
        packs = lambda c: [
            vm(c, cx // 2, 8, 128), vm(c, cx // 2, 8, 128),
            vm(c, ex // 2, 8, 128), vm(c, ex // 2, 8, 128),
        ]
        field = (3, ex, ey, 128)
        dma = pltpu.SemaphoreType.DMA
        return pl.pallas_call(
            functools.partial(kernel, (nx, ny, nz, cx, cy, vectors, order)),
            out_shape=[jax.ShapeDtypeStruct(forces.shape, f32)] * 3,
            in_specs=[pl.BlockSpec(memory_space=pltpu.VMEM)] * 5,
            out_specs=[pl.BlockSpec(memory_space=pltpu.VMEM)] * 3,
            scratch_shapes=[
                vm(*field), vm(*field), vm(*field), vm(ex, ey, 128), vm(1, ex, ey, 128),
                vm(*field), vm(*field), vm(*field), vm(*field), vm(ex, ey, 128),
                *packs(3), *packs(3), *packs(1),
                vm(3, 2, 3, ey, 128), vm(3, 2, 3, ey, 128), vm(2, ey, 128),
                vm(nz, slab, order), vm(order // BLOCK, BLOCK, BLOCK), vm(order, order),
                vm(2, 2, 128), vm(2, n, 2, 128), vm(n // 8, 1, 128), vm(n // 8, 1, 128),
                dma((8,)), dma((8,)), dma((8,)), dma((8,)), dma((8,)), dma((8,)),
                dma((3, 2)), dma((3, 2)), dma((2,)), dma((2, n)),
                dma((max(nz - 1, 1),)), dma((max(nz - 1, 1),)), dma,
            ],
            compiler_params=pltpu.CompilerParams(
                collective_id=0, has_side_effects=True, vmem_limit_bytes=66 * 1000 * 1000
            ),
        )(forces, mass_shift, deflation, coarse_factor, slot_column)

    return jax.shard_map(
        body,
        mesh=mesh,
        in_specs=(
            P(None, "gx", "gy", "gz"),
            P("gx", "gy", "gz"),
            P(None, None, "gx", "gy", "gz"),
            P("gz", None),
            P(),
        ),
        out_specs=(P(None, "gx", "gy", "gz"), P(None, "gx", "gy", "gz"), P(None, "gx", "gy", "gz")),
        check_vma=False,
    )
```

```python
import functools

import jax
import jax.numpy as jnp
from jax import lax
from jax.experimental import pallas as pl
from jax.experimental.pallas import tpu as pltpu
from jax.sharding import PartitionSpec as P

SWEEPS = 3
ITERS = 4
MESH = pl.DeviceIdType.MESH
HIGHEST = lax.Precision.HIGHEST
W = 3
LEAD = 4
DIRS = tuple((dx, dy) for dx in (-1, 0, 1) for dy in (-1, 0, 1) if (dx, dy) != (0, 0))
BLOCK = 128


def dot(a, b):
    return jnp.dot(a, b, precision=HIGHEST, preferred_element_type=jnp.float32)


def kernel(
    sizes,
    forces, mass, defl_hbm, factor, slot_column,
    sol, res, direc,
    zext, rext, idir, cext, mext, cor, ua, ub, uz, vx,
    low, high, got_low, got_high,
    low_c, high_c, got_low_c, got_high_c,
    low_m, high_m, got_low_m, got_high_m,
    zsend, zgot, vzb, defl,
    full, inv, sol_mat, gsend, gat, gres, gdir,
    zx_send, zx_recv, c_send, c_recv, m_send, m_recv,
    zc_send, zc_recv, g_send, g_recv, f_send, f_recv, f_local, d_local,
):
    nx, ny, nz, cx, cy, vectors, order = sizes
    n = nx * ny * nz
    ex = cx + 2 * LEAD
    ey = cy + 8
    gx, gy, gz = lax.axis_index("gx"), lax.axis_index("gy"), lax.axis_index("gz")
    me = (gx * ny + gy) * nz + gz
    f32 = jnp.float32

    def coords(t):
        return {"gx": t // (ny * nz), "gy": (t // nz) % ny, "gz": t % nz}

    lane = lax.broadcasted_iota(jnp.int32, (ey, 128), 1)
    row8 = lax.broadcasted_iota(jnp.int32, (8, 128), 0)
    rows = lax.broadcasted_iota(jnp.int32, (ey, 128), 0)
    lane1 = lax.broadcasted_iota(jnp.int32, (1, 128), 1)

    load = pltpu.make_async_copy(defl_hbm, defl, d_local)
    load.start()
    for ref in (
        zext.at[0], zext.at[1], got_low.at[0], got_low.at[1], got_high.at[0], got_high.at[1],
        cor, mext, got_low_c, got_high_c, got_low_m, got_high_m,
    ):
        lead = ref.shape[0]
        for c in range(lead):
            def clear(i, _, ref=ref, c=c):
                ref[c, i] = jnp.zeros(ref.shape[2:], f32)
                return 0
            lax.fori_loop(0, ref.shape[1], clear, 0)
    zgot[...] = jnp.zeros(zgot.shape, f32)

    barrier = pltpu.get_barrier_semaphore()

    def greet(j, _):
        t = lax.rem(me + j, n)
        pl.semaphore_signal(barrier, inc=1, device_id=coords(t), device_id_type=MESH)
        return 0

    lax.fori_loop(1, n, greet, 0)
    pl.semaphore_wait(barrier, n - 1)

    slab = order // nz

    def slab_copy(j):
        t = lax.rem(gz + j, nz)
        return pltpu.make_async_remote_copy(
            src_ref=factor,
            dst_ref=full.at[gz],
            send_sem=f_send.at[j - 1],
            recv_sem=f_recv.at[j - 1],
            device_id={"gx": gx, "gy": gy, "gz": t},
            device_id_type=MESH,
        )

    for j in range(1, nz):
        slab_copy(j).start()
    own_slab = pltpu.make_async_copy(factor, full.at[gz], f_local)
    own_slab.start()

    def exists(dx, dy):
        ok = jnp.bool_(True)
        if dx < 0:
            ok = jnp.logical_and(ok, gx > 0)
        if dx > 0:
            ok = jnp.logical_and(ok, gx < nx - 1)
        if dy < 0:
            ok = jnp.logical_and(ok, gy > 0)
        if dy > 0:
            ok = jnp.logical_and(ok, gy < ny - 1)
        return ok

    def pieces(ext, lo, hi, glo, ghi, send, recv):
        half = cx // 2
        out = []
        for d, (dx, dy) in enumerate(DIRS):
            if dy == 0:
                src = ext.at[:, pl.ds(LEAD if dx < 0 else LEAD + cx - W, W), pl.ds(0, cy)]
                dst = ext.at[:, pl.ds(LEAD + cx if dx < 0 else LEAD - W, W), pl.ds(0, cy)]
            else:
                start, count = {0: (0, half), -1: (0, 2), 1: (half - 2, 2)}[dx]
                to = {0: 2, -1: 2 + half, 1: 0}[dx]
                src = (lo if dy < 0 else hi).at[:, pl.ds(start, count)]
                dst = (glo if dy < 0 else ghi).at[:, pl.ds(to, count)]
            copy = pltpu.make_async_remote_copy(
                src_ref=src,
                dst_ref=dst,
                send_sem=send.at[d],
                recv_sem=recv.at[d],
                device_id={"gx": gx + dx, "gy": gy + dy, "gz": gz},
                device_id_type=MESH,
            )
            out.append((dx, dy, copy))
        return out

    def send_halo(ext, lo, hi, glo, ghi, send, recv):
        def pack(i, _):
            for c in range(ext.shape[0]):
                even, odd = LEAD + 2 * i, LEAD + 2 * i + 1
                lo[c, i] = jnp.where(row8 < 4, ext[c, even, 0:8], pltpu.roll(ext[c, odd, 0:8], 4, 0))
                hi[c, i] = jnp.where(
                    row8 >= 4, ext[c, even, cy - 8 : cy], pltpu.roll(ext[c, odd, cy - 8 : cy], 4, 0)
                )
            return 0

        lax.fori_loop(0, cx // 2, pack, 0)
        for dx, dy, copy in pieces(ext, lo, hi, glo, ghi, send, recv):
            pl.when(exists(dx, dy))(copy.start)

    def take_halo(ext, lo, hi, glo, ghi, send, recv):
        for dx, dy, copy in pieces(ext, lo, hi, glo, ghi, send, recv):
            pl.when(exists(-dx, -dy))(copy.wait_recv)
            pl.when(exists(dx, dy))(copy.wait_send)

        def unpack(i, _):
            for c in range(ext.shape[0]):
                a, b = glo[c, i], ghi[c, i]
                ext[c, 2 * i, cy : cy + 8] = jnp.where(row8 < 4, a, b)
                ext[c, 2 * i + 1, cy : cy + 8] = jnp.where(
                    row8 < 4, pltpu.roll(a, 4, 0), pltpu.roll(b, 4, 0)
                )
            return 0

        lax.fori_loop(0, ex // 2, unpack, 0)

    def halo_z(slot):
        return (
            zext.at[slot], low, high, got_low.at[slot], got_high.at[slot],
            zx_send, zx_recv.at[slot],
        )

    halo_m = (mext, low_m, high_m, got_low_m, got_high_m, m_send, m_recv)

    eighth = cx // 8

    def thin_pieces():
        out = []
        for d, (dx, dy) in enumerate(DIRS):
            if dy == 0:
                src = cor.at[:, pl.ds(LEAD if dx < 0 else LEAD + cx - 1, 1), pl.ds(0, cy)]
                dst = cor.at[:, pl.ds(LEAD + cx if dx < 0 else LEAD - 1, 1), pl.ds(0, cy)]
            else:
                start, count = {0: (0, eighth), -1: (0, 1), 1: (eighth - 1, 1)}[dx]
                to = {0: 1, -1: 1 + eighth, 1: 0}[dx]
                src = (low_c if dy < 0 else high_c).at[:, pl.ds(start, count)]
                dst = (got_low_c if dy < 0 else got_high_c).at[:, pl.ds(to, count)]
            copy = pltpu.make_async_remote_copy(
                src_ref=src,
                dst_ref=dst,
                send_sem=c_send.at[d],
                recv_sem=c_recv.at[d],
                device_id={"gx": gx + dx, "gy": gy + dy, "gz": gz},
                device_id_type=MESH,
            )
            out.append((dx, dy, copy))
        return out

    def send_thin():
        for c in range(3):
            for t in range(eighth):
                lo = hi = jnp.zeros((8, 128), f32)
                for j in range(8):
                    x = LEAD + 8 * t + j
                    lo = jnp.where(row8 == j, pltpu.roll(cor[c, x, 0:8], j, 0) if j else cor[c, x, 0:8], lo)
                    a = cor[c, x, cy - 8 : cy]
                    hi = jnp.where(row8 == j, pltpu.roll(a, (j + 1) % 8, 0) if j < 7 else a, hi)
                low_c[c, t] = lo
                high_c[c, t] = hi
        for dx, dy, copy in thin_pieces():
            pl.when(exists(dx, dy))(copy.start)

    def take_thin():
        for dx, dy, copy in thin_pieces():
            pl.when(exists(-dx, -dy))(copy.wait_recv)
            pl.when(exists(dx, dy))(copy.wait_send)
        for c in range(3):
            for t in range(eighth + 2):
                a, b = got_low_c[c, t], got_high_c[c, t]
                for j in range(8):
                    x = LEAD - 8 + 8 * t + j
                    if LEAD - 1 <= x <= LEAD + cx:
                        p = pltpu.roll(a, 8 - j, 0) if j else a
                        q = pltpu.roll(b, 7 - j, 0) if j < 7 else b
                        cor[c, x, cy : cy + 8] = jnp.where(row8 < 4, p, q)

    def columns(stage, side):
        return pltpu.make_async_remote_copy(
            src_ref=zsend.at[stage, side],
            dst_ref=zgot.at[stage, 1 - side],
            send_sem=zc_send.at[stage, side],
            recv_sem=zc_recv.at[stage, side],
            device_id={"gx": gx, "gy": gy, "gz": gz + (2 * side - 1)},
            device_id_type=MESH,
        )

    has = (gz > 0, gz < nz - 1)

    def send_columns(u, stage, first, last):
        for side in (0, 1):
            @pl.when(has[side])
            def _(side=side):
                def gather(x, acc):
                    shift = x if side == 0 else x + 1
                    return tuple(
                        jnp.where(lane == x, pltpu.roll(u[c, x], shift, 1), acc[c]) for c in range(3)
                    )

                acc = lax.fori_loop(first, last, gather, (jnp.zeros((ey, 128), f32),) * 3, unroll=2)
                for c in range(3):
                    zsend[stage, side, c] = acc[c]
                columns(stage, side).start()

    def take_columns(stage):
        for side in (0, 1):
            pl.when(has[1 - side])(columns(stage, side).wait_recv)
            pl.when(has[side])(columns(stage, side).wait_send)
        for side in (0, 1):
            bx, by = zgot[stage, side, 0], zgot[stage, side, 1]
            vzb[side] = (
                pltpu.roll(bx, 127, 1) - pltpu.roll(bx, 1, 1)
                + pltpu.roll(by, ey - 1, 0) - pltpu.roll(by, 1, 0)
            )

    def exchange_columns(u, stage, first, last):
        send_columns(u, stage, first, last)
        take_columns(stage)

    def y_pair(v):
        return pltpu.roll(v, ey - 1, 0), pltpu.roll(v, 1, 0)

    def z_pair(v, upper, lower, x):
        up = jnp.where(lane == 127, pltpu.roll(upper, 127 - x, 1), pltpu.roll(v, 127, 1))
        down = jnp.where(lane == 0, pltpu.roll(lower, 128 - x, 1), pltpu.roll(v, 1, 1))
        return up, down

    def off_diagonal(u, stage, first, last, use, carry):
        def before(x, _):
            p, m = y_pair(u[1, x])
            q, r = z_pair(u[2, x], zgot[stage, 1, 2], zgot[stage, 0, 2], x)
            vx[x] = (p - m) + (q - r)
            return 0

        lax.fori_loop(first - 1, last + 1, before, 0, unroll=2)

        def at(x, carry):
            pair, diff = [], []
            for c in range(3):
                v = u[c, x]
                xp, xm = u[c, x + 1], u[c, x - 1]
                yp, ym = y_pair(v)
                zp, zm = z_pair(v, zgot[stage, 1, c], zgot[stage, 0, c], x)
                pair.append((xp + xm, yp + ym, zp + zm))
                diff.append(((xp - xm), (yp - ym), (zp - zm))[c])
            px, py, pz = diff
            dx = vx[x + 1] - vx[x - 1]
            yp, ym = y_pair(px + pz)
            zp, zm = z_pair(px + py, vzb[1], vzb[0], x)
            mixed = (dx, yp - ym, zp - zm)
            off = tuple(
                0.25 * (pair[c][0] + pair[c][1] + pair[c][2]) + 0.625 * pair[c][c] + 0.15625 * mixed[c]
                for c in range(3)
            )
            return use(x, off, carry)

        return lax.fori_loop(first, last, at, carry)

    base = lax.rem(me, 8) * vectors if vectors * 8 == 128 else 0

    def share(slot, gamma, energy):
        def part(x, acc):
            acc = list(acc)
            for c in range(3):
                v = zext[slot, c, LEAD + x, 0:cy]
                for k in range(vectors):
                    prod = defl[k, c, x] * v
                    for t in range(0, cy, 8):
                        acc[k] = acc[k] + prod[t : t + 8]
            return tuple(acc)

        acc = lax.fori_loop(0, cx, part, (jnp.zeros((8, 128), f32),) * vectors)
        line = jnp.zeros((1, 128), f32)
        for k in range(vectors):
            total = jnp.sum(jnp.sum(acc[k], axis=0, keepdims=True), axis=1, keepdims=True)
            line = jnp.where(lane1 == base + k, total, line)
        gsend[slot, 0:1] = line
        gsend[slot, 1:2] = jnp.where(lane1 == 0, gamma, jnp.where(lane1 == 1, energy, 0.0))
        gat[slot, me] = gsend[slot]

        def push(j, _):
            t = lax.rem(me + j, n)
            pltpu.make_async_remote_copy(
                src_ref=gsend.at[slot],
                dst_ref=gat.at[slot, me],
                send_sem=g_send.at[slot],
                recv_sem=g_recv.at[slot, me],
                device_id=coords(t),
                device_id_type=MESH,
            ).start()
            return 0

        lax.fori_loop(1, n, push, 0)

    def collect(slot):
        def await_one(j, _):
            t = lax.rem(me + j, n)
            pltpu.make_async_copy(gsend.at[slot], gat.at[slot, t], g_recv.at[slot, t]).wait()
            return 0

        lax.fori_loop(1, n, await_one, 0)
        pltpu.make_async_copy(
            gat.at[slot, pl.ds(0, n - 1)], gat.at[slot, pl.ds(0, n - 1)], g_send.at[slot]
        ).wait()
        lines, scal = [], jnp.zeros((1, 128), f32)
        for t in range(n // 8):
            both = jnp.zeros((2, 128), f32)
            for s in range(8):
                both = both + gat[slot, 8 * t + s]
            lines.append(both[0:1])
            scal = scal + both[1:2]
        gamma = jnp.sum(jnp.where(lane1 == 0, scal, 0.0), axis=1, keepdims=True)
        energy = jnp.sum(jnp.where(lane1 == 1, scal, 0.0), axis=1, keepdims=True)
        return lines, gamma, energy

    def fill(x, _):
        for c in range(3):
            zext[0, c, LEAD + x, 0:cy] = forces[c, x]
            sol[c, x] = jnp.zeros((cy, 128), f32)
            direc[c, x] = jnp.zeros((cy, 128), f32)
        mext[0, LEAD + x, 0:cy] = mass[x]
        return 0

    lax.fori_loop(0, cx, fill, 0)
    send_halo(*halo_z(0))
    send_halo(*halo_m)
    load.wait()
    zero = jnp.zeros((1, 1), f32)
    share(0, zero, zero)

    for j in range(1, nz):
        copy = slab_copy(j)
        copy.wait_recv()
        copy.wait_send()
    own_slab.wait()
    per_slab = slab // BLOCK
    blocks = order // BLOCK
    group = min(4, blocks)
    r_i = lax.broadcasted_iota(jnp.int32, (BLOCK, BLOCK), 0)
    c_i = lax.broadcasted_iota(jnp.int32, (BLOCK, BLOCK), 1)

    def invert(g, _):
        lows, xs = [], []
        for q in range(group):
            i = g * group + q
            at = pl.ds(pl.multiple_of((i % per_slab) * BLOCK, BLOCK), BLOCK)
            col = pl.ds(pl.multiple_of(i * BLOCK, BLOCK), BLOCK)
            block = full[i // per_slab, at, col]
            lows.append(block)
            xs.append(jnp.where(r_i == c_i, 1.0 / jnp.where(r_i == c_i, block, 1.0), 0.0))
        s = 1
        while s < BLOCK:
            pick = (r_i // (2 * s) == c_i // (2 * s)) & ((r_i // s) % 2 == 1) & ((c_i // s) % 2 == 0)
            mids = [dot(jnp.where(pick, lows[q], 0.0), xs[q]) for q in range(group)]
            xs = [xs[q] - dot(xs[q], mids[q]) for q in range(group)]
            s *= 2
        for q in range(group):
            inv[g * group + q] = xs[q]
        return 0

    lax.fori_loop(0, blocks // group, invert, 0)

    width = min(512, order)

    def wipe(i, _):
        sol_mat[pl.ds(pl.multiple_of(i * 8, 8), 8), :] = jnp.zeros((8, order), f32)
        return 0

    lax.fori_loop(0, order // 8, wipe, 0)
    w_rows = lax.broadcasted_iota(jnp.int32, (BLOCK, width), 0)

    def substitute(i, _):
        at = pl.ds(pl.multiple_of((i % per_slab) * BLOCK, BLOCK), BLOCK)

        def over(j, _):
            col = pl.ds(pl.multiple_of(j * width, width), width)
            right = jnp.where(w_rows + i * BLOCK == slot_column[:, col], 1.0, 0.0)
            right = right - dot(full[i // per_slab, at, :], sol_mat[:, col])
            sol_mat[pl.ds(pl.multiple_of(i * BLOCK, BLOCK), BLOCK), col] = dot(inv[i], right)
            return 0

        lax.fori_loop(0, order // width, over, 0)
        return 0

    lax.fori_loop(0, blocks, substitute, 0)

    lines, _, _ = collect(0)
    for t in range(n // 8):
        gres[t] = lines[t]
        gdir[t] = jnp.zeros((1, 128), f32)

    strip = 64

    def coarse():
        own = pl.ds(pl.multiple_of((me // 8) * 128, 128), 128)

        def some(i, acc):
            at = pl.ds(pl.multiple_of(i * strip, strip), strip)
            y = jnp.zeros((strip, 128), f32)
            for t in range(order // 128):
                y = y + sol_mat[at, t * 128 : (t + 1) * 128] * gres[t]
            y = jnp.sum(y, axis=1, keepdims=True)
            return acc + jnp.sum(y * sol_mat[at, own], axis=0, keepdims=True)

        line = lax.fori_loop(0, order // strip, some, jnp.zeros((1, 128), f32), unroll=2)
        weights = [
            jnp.sum(jnp.where(lane1 == base + k, line, 0.0), axis=1, keepdims=True)
            for k in range(vectors)
        ]
        spread = [jnp.broadcast_to(w, (8, 128)) for w in weights]

        def correct(x, _):
            for c in range(3):
                for t in range(0, cy, 8):
                    acc = spread[0] * defl[0, c, x, t : t + 8]
                    for k in range(1, vectors):
                        acc = acc + spread[k] * defl[k, c, x, t : t + 8]
                    cor[c, LEAD + x, t : t + 8] = acc
            return 0

        lax.fori_loop(0, cx, correct, 0)

    coarse()
    send_thin()
    take_halo(*halo_z(0))
    take_halo(*halo_m)
    y_ok = (rows < cy) | ((rows < cy + 4) & (gy < ny - 1)) | ((rows >= cy + 4) & (gy > 0))

    def settle(x, _):
        x_ok = ((x >= LEAD) | (gx > 0)) & ((x < LEAD + cx) | (gx < nx - 1))
        keep = jnp.where(x_ok, 1.0, 0.0)
        cext[x] = jnp.where(y_ok, 0.6 / (mext[0, x] + 2.75), 0.0) * keep
        for c in range(3):
            rext[c, x] = zext[0, c, x]
            idir[c, x] = jnp.zeros((ey, 128), f32)
        return 0

    lax.fori_loop(0, ex, settle, 0)

    def iterate(it, carry):
        gamma_prior, step_prior = carry
        slot = lax.rem(it + 1, 2)
        def start(x, _):
            for c in range(3):
                ua[c, x] = cext[x] * rext[c, x]
            return 0

        lax.fori_loop(LEAD - 3, LEAD + cx + 3, start, 0)

        def sweep(src, dst):
            def use(x, off, carry):
                for c in range(3):
                    dst[c, x] = 0.4 * src[c, x] + cext[x] * (rext[c, x] + off[c])
                return carry
            return use

        exchange_columns(ua, 0, LEAD - 3, LEAD + cx + 3)
        off_diagonal(ua, 0, LEAD - 2, LEAD + cx + 2, sweep(ua, ub), 0)
        exchange_columns(ub, 1, LEAD - 2, LEAD + cx + 2)
        off_diagonal(ub, 1, LEAD - 1, LEAD + cx + 1, sweep(ub, uz), 0)
        take_thin()

        def join(x, _):
            for c in range(3):
                uz[c, x] = uz[c, x] + cor[c, x]
            return 0

        lax.fori_loop(LEAD - 1, LEAD + cx + 1, join, 0)
        exchange_columns(uz, 2, LEAD - 1, LEAD + cx + 1)

        def image(x, off, carry):
            gam, ene = carry
            diag = mext[0, x, 0:cy] + 2.75
            for c in range(3):
                z = uz[c, x, 0:cy]
                a = diag * z - off[c][0:cy]
                zext[slot, c, x, 0:cy] = a
                gam = gam + rext[c, x, 0:cy] * z
                ene = ene + z * a
            return gam, ene

        nothing = jnp.zeros((cy, 128), f32)
        gam, ene = off_diagonal(uz, 2, LEAD, LEAD + cx, image, (nothing, nothing))
        gam = jnp.sum(jnp.sum(gam, axis=0, keepdims=True), axis=1, keepdims=True)
        ene = jnp.sum(jnp.sum(ene, axis=0, keepdims=True), axis=1, keepdims=True)

        @pl.when(it < ITERS - 1)
        def _():
            send_halo(*halo_z(slot))

        share(slot, gam, ene)
        lines, gamma, energy = collect(slot)
        momentum = jnp.where(it == 0, 0.0, gamma / gamma_prior)
        step = gamma / (energy - momentum * gamma / step_prior)

        for t in range(n // 8):
            image_line = lines[t] + momentum * gdir[t]
            gdir[t] = image_line
            gres[t] = gres[t] - step * image_line

        @pl.when(it < ITERS - 1)
        def _():
            coarse()
            send_thin()

        def advance(x, _):
            for c in range(3):
                d = uz[c, LEAD + x, 0:cy] + momentum * direc[c, x]
                direc[c, x] = d
                sol[c, x] = sol[c, x] + step * d
            return 0

        lax.fori_loop(0, cx, advance, 0)

        @pl.when(it < ITERS - 1)
        def _():
            take_halo(*halo_z(slot))

        def update(x, _):
            for c in range(3):
                image_dir = zext[slot, c, x] + momentum * idir[c, x]
                idir[c, x] = image_dir
                rext[c, x] = rext[c, x] - step * image_dir
            return 0

        lax.fori_loop(LEAD - 3, LEAD + cx + 3, update, 0)
        return gamma, step

    one = jnp.ones((1, 1), f32)
    lax.fori_loop(0, ITERS, iterate, (one, one))

    def give(x, _):
        for c in range(3):
            res[c, x] = rext[c, LEAD + x, 0:cy]
        return 0

    lax.fori_loop(0, cx, give, 0)


def solution(mesh):
    nx, ny, nz = mesh.shape["gx"], mesh.shape["gy"], mesh.shape["gz"]

    def body(forces, mass_shift, deflation, coarse_factor, coarse_slot):
        vectors = deflation.shape[0]
        cx, cy = forces.shape[1], forces.shape[2]
        order = coarse_factor.shape[1]
        slab = coarse_factor.shape[0]
        n = nx * ny * nz
        slot_column = (
            coarse_slot[:, None] * vectors + jnp.arange(vectors, dtype=jnp.int32)[None, :]
        ).reshape(1, -1)
        ex, ey = cx + 2 * LEAD, cy + 8
        f32 = jnp.float32
        vm = lambda *shape: pltpu.VMEM(shape, f32)
        packs = lambda c: [
            vm(c, cx // 2, 8, 128), vm(c, cx // 2, 8, 128),
            vm(c, ex // 2, 8, 128), vm(c, ex // 2, 8, 128),
        ]
        field = (3, ex, ey, 128)
        dma = pltpu.SemaphoreType.DMA
        return pl.pallas_call(
            functools.partial(kernel, (nx, ny, nz, cx, cy, vectors, order)),
            out_shape=[jax.ShapeDtypeStruct(forces.shape, f32)] * 3,
            in_specs=[
                pl.BlockSpec(memory_space=pl.ANY if i == 2 else pltpu.VMEM) for i in range(5)
            ],
            out_specs=[pl.BlockSpec(memory_space=pltpu.VMEM)] * 3,
            scratch_shapes=[
                vm(2, *field), vm(*field), vm(*field), vm(ex, ey, 128), vm(1, ex, ey, 128),
                vm(*field), vm(*field), vm(*field), vm(*field), vm(ex, ey, 128),
                vm(3, cx // 2, 8, 128), vm(3, cx // 2, 8, 128),
                vm(2, 3, ex // 2, 8, 128), vm(2, 3, ex // 2, 8, 128),
                vm(3, cx // 8, 8, 128), vm(3, cx // 8, 8, 128),
                vm(3, cx // 8 + 2, 8, 128), vm(3, cx // 8 + 2, 8, 128),
                *packs(1),
                vm(3, 2, 3, ey, 128), vm(3, 2, 3, ey, 128), vm(2, ey, 128), vm(*deflation.shape),
                vm(nz, slab, order), vm(order // BLOCK, BLOCK, BLOCK), vm(order, order),
                vm(2, 2, 128), vm(2, n, 2, 128), vm(n // 8, 1, 128), vm(n // 8, 1, 128),
                dma((8,)), dma((2, 8)), dma((8,)), dma((8,)), dma((8,)), dma((8,)),
                dma((3, 2)), dma((3, 2)), dma((2,)), dma((2, n)),
                dma((max(nz - 1, 1),)), dma((max(nz - 1, 1),)), dma, dma,
            ],
            compiler_params=pltpu.CompilerParams(
                collective_id=0, has_side_effects=True, vmem_limit_bytes=66 * 1000 * 1000
            ),
        )(forces, mass_shift, deflation, coarse_factor, slot_column)

    return jax.shard_map(
        body,
        mesh=mesh,
        in_specs=(
            P(None, "gx", "gy", "gz"),
            P("gx", "gy", "gz"),
            P(None, None, "gx", "gy", "gz"),
            P("gz", None),
            P(),
        ),
        out_specs=(P(None, "gx", "gy", "gz"), P(None, "gx", "gy", "gz"), P(None, "gx", "gy", "gz")),
        check_vma=False,
    )
```
